32 devices in a mesh: groups: 2 (over y), pts: 4 (over z), cb: 4 (over x, core).
Axes of the slice: x: 2, y: 2, z: 4, core: 2. Of those that a mesh axis runs over, the one named last changes fastest.
Arguments:
- points: bfloat16 [16384, 768], P(('groups', 'pts')), parts along dimension 0, may hold values from -60 to 60
- code_one: int32 [16384], P(('groups', 'pts')), parts along dimension 0, may hold values from 0 to 2047
- code_two: int32 [16384], P(('groups', 'pts')), parts along dimension 0, may hold values from 0 to 2047
- cent_one: bfloat16 [4096, 768], P(('groups', 'cb')), parts along dimension 0, may hold values from -6 to 6
- cent_two: bfloat16 [4096, 768], P(('groups', 'cb')), parts along dimension 0, may hold values from -6 to 6
Outputs:
- new_one: bfloat16 [4096, 768], P(('groups', 'cb')), parts along dimension 0
- new_two: bfloat16 [4096, 768], P(('groups', 'cb')), parts along dimension 0
- distortion: float32 [4], P('groups'), parts along dimension 0
The draws below stay inside these ranges and needn't reach their ends.
There are 2 independent parts, one for each index of `groups`. The reference program is written for one: setup_inputs(seed, part) draws one part's arguments, and reference() takes and returns one part's arrays. A program takes and returns all parts, laid end to end along the dimension named above; each array names one. Nothing has to cross between parts.
All inputs are finite; a program needn't handle non-finite values.
Results may differ from the reference program's by a relative error of at most 0.0014.
Values may be sent and summed in bfloat16 or wider, within the bound.
A program may use at most 64 MiB of HBM per device.

```python
import math
import jax
import jax.numpy as jnp
from jax import lax

D = 768
K = 2048
POINTS = 8192


def centre_table(key):
    values = jax.random.normal(jax.random.fold_in(key, 11), (K, D), jnp.float32)
    return jnp.clip(values, -6.0, 6.0).astype(jnp.bfloat16)


def draw_cent_one(key, part):
    return centre_table(key)


def draw_points(key, part):
    centres = centre_table(key).astype(jnp.float32)
    picks = jax.random.randint(jax.random.fold_in(key, 12), (POINTS,), 0, K)
    chosen = jnp.take(centres, picks, axis=0)
    key_jit = jax.random.fold_in(jax.random.fold_in(key, 13), 0)
    key_base = jax.random.fold_in(jax.random.fold_in(key, 13), 1)
    key_cols = jax.random.fold_in(jax.random.fold_in(key, 13), 3)
    rowpos = jnp.arange(POINTS, dtype=jnp.float32) / POINTS
    trend = jnp.power(3.0, rowpos)
    jitter = jnp.exp(jax.random.uniform(key_jit, (POINTS,), jnp.float32, 0.0, math.log(4.0)))
    colscale = jnp.exp(jax.random.uniform(key_cols, (D,), jnp.float32, math.log(0.5), math.log(2.0)))
    base = jax.random.normal(key_base, (POINTS, D), jnp.float32)
    noise = 0.15 * base * (trend * jitter)[:, None] * colscale[None, :]
    return jnp.clip(chosen + noise, -60.0, 60.0).astype(jnp.bfloat16)


def plant(result, own_key, smallest, high):
    shape = result.shape
    place = [jax.random.randint(jax.random.fold_in(own_key, axis), (), 0, shape[axis]) for axis in range(len(shape))]
    result = result.at[tuple(place)].set(smallest)
    longest = shape.index(max(shape))
    place[longest] = (place[longest] + 1) % shape[longest]
    return result.at[tuple(place)].set(high)


def levels(stream_key, shape, cuts, smallest, top_value):
    def one(axis_at, parts):
        steps = jax.random.uniform(jax.random.fold_in(jax.random.fold_in(stream_key, 6), axis_at), (parts,), jnp.float32, smallest / len(cuts), top_value / len(cuts))
        return jnp.repeat(jnp.exp(steps), shape[axis_at] // parts).reshape((-1,) + (1,) * (len(shape) - axis_at - 1))

    level = one(*cuts[0])
    for cut in cuts[1:]:
        level = level * one(*cut)
    return level


def normal_values(key, dims, scale, limit, cuts=(), kind=jnp.bfloat16):
    level = levels(key, dims, cuts, -0.22, 0.18) if cuts else 1.0
    result = jax.random.normal(key, dims, jnp.float32) * scale * level
    return jnp.minimum(jnp.maximum(result, -limit), limit).astype(kind)


def setup_inputs(seed: int = 0, part: int = 0) -> dict:
    keys = jax.random.split(jax.random.key(seed), 6)
    part_keys = jax.random.split(jax.random.fold_in(keys[5], part), 6)
    return {
        "points": draw_points(jax.random.fold_in(jax.random.fold_in(keys[5], part), 71), part),
        "code_one": plant(jax.random.randint(part_keys[1], (POINTS,), 0, K), jax.random.fold_in(part_keys[1], 1), 0, K - 1).astype(jnp.int32),
        "code_two": plant(jax.random.randint(part_keys[2], (POINTS,), 0, K), jax.random.fold_in(part_keys[2], 1), 0, K - 1).astype(jnp.int32),
        "cent_one": draw_cent_one(jax.random.fold_in(jax.random.fold_in(keys[5], part), 71), part),
        "cent_two": normal_values(part_keys[4], (K, D), 1.0, 6.0, ((0, 4),)),
    }


def nearest_total(data, cents):
    csq = jnp.sum(jnp.square(cents.astype(jnp.float32)), axis=1)
    block = math.gcd(POINTS, 4096)
    blocks = data.reshape(POINTS // block, block, D)

    def one_block(rows_in):
        sq = jnp.sum(jnp.square(rows_in.astype(jnp.float32)), axis=1)
        cross = lax.dot_general(rows_in, cents, (((1,), (1,)), ((), ())), preferred_element_type=jnp.float32)
        dist = sq[:, None] - 2.0 * cross + csq[None, :]
        return jnp.min(dist, axis=1)

    mins = lax.map(one_block, blocks)
    return jnp.sum(mins)


def update(data, codes, cents):
    sums = jax.ops.segment_sum(data.astype(jnp.float32), codes, num_segments=K)
    counts = jax.ops.segment_sum(jnp.ones((POINTS,), jnp.float32), codes, num_segments=K)
    return ((sums + cents.astype(jnp.float32)) / (counts + 1.0)[:, None]).astype(jnp.bfloat16)


def reference(points, code_one, code_two, cent_one, cent_two):
    new_one = update(points, code_one, cent_one)
    looked = jnp.take(new_one, code_one, axis=0)
    residual = (points.astype(jnp.float32) - looked.astype(jnp.float32)).astype(jnp.bfloat16)
    new_two = update(residual, code_two, cent_two)
    first = nearest_total(points, cent_one)
    second = nearest_total(residual, cent_two)
    distortion = jnp.stack([first, second]) / jnp.float32(POINTS * D)
    return new_one, new_two, distortion
```

```python
import functools

import jax
import jax.numpy as jnp
from jax import lax
from jax.experimental import pallas as pl
from jax.experimental.pallas import tpu as pltpu
from jax.sharding import PartitionSpec as P

F32 = jnp.float32
BF16 = jnp.bfloat16
I16 = jnp.int16
CORES = 2
SIZE = 32
SPAN = 128
GROUP = 64
PIECES = 8
HOP = 3
TOP = 32700.0
TINY = 2.0 ** -100
LOWEST = -16
BITS = 7


def fused_kernel(
    npts, ncb,
    points, code_one, code_two, cent_one, cent_two,
    new_one, new_two, total_out,
    residual, codebook, sums, quant, quant_in, meta, meta_in, cols, ones, column,
    mins, mins_in, tot, tot_in, scaled, csq, squares,
    up_send, up_recv, swap_send, swap_recv, down_send, down_recv,
    mup_send, mup_recv, mswap_send, mswap_recv,
    x_send, x_recv, d_send, d_recv, min_send, min_recv, tot_send, tot_recv,
):
    p = lax.axis_index("pts")
    c = lax.axis_index("cb")
    npoints, width = points.shape
    rows = cent_one.shape[0]
    n = rows // SIZE
    per = SPAN // SIZE
    nx = ncb // CORES
    cx, cc = c // CORES, c % CORES
    sibling = cx * CORES + (1 - cc)
    side = p // 2
    inner = jnp.logical_or(p == 1, p == 2)
    outer = jnp.logical_not(inner)
    pair = p + 1 - 2 * (p % 2)
    across = npts - 1 - p

    def to(axis, src, dst, s, r, where):
        return pltpu.make_async_remote_copy(
            src_ref=src, dst_ref=dst, send_sem=s, recv_sem=r,
            device_id={axis: where}, device_id_type=pl.DeviceIdType.MESH,
        )

    barrier = pltpu.get_barrier_semaphore()
    for d in range(1, npts):
        pl.semaphore_signal(barrier, inc=1, device_id={"pts": (p + d) % npts},
                            device_id_type=pl.DeviceIdType.MESH)
    for d in range(1, ncb):
        pl.semaphore_signal(barrier, inc=1, device_id={"cb": (c + d) % ncb},
                            device_id_type=pl.DeviceIdType.MESH)

    def span(start, length):
        return pl.ds(pl.multiple_of(start, length), length)

    def chunk(j):
        return span(j * SIZE, SIZE)

    def up(k, j):
        return to("pts", quant.at[k, side, chunk(j), :], quant_in.at[k, chunk(j), :],
                  up_send.at[k, j], up_recv.at[k, j], pair)

    def swap(k, j):
        ref = quant.at[k, side, chunk(j), :]
        return to("pts", ref, ref, swap_send.at[k, j], swap_recv.at[k, j], across)

    def meta_up(k, t):
        return to("pts", meta.at[k, side, t], meta_in.at[k, t], mup_send.at[k, t],
                  mup_recv.at[k, t], pair)

    def meta_swap(k, t):
        ref = meta.at[k, side, t]
        return to("pts", ref, ref, mswap_send.at[k, t], mswap_recv.at[k, t], across)

    def block(col, j):
        first = j * SIZE
        at = (first // GROUP) * (GROUP * ncb) + col * GROUP + first % GROUP
        return codebook.at[span(at, SIZE), :]

    def fresh(k, j):
        return block(c, j) if k == 0 else new_two.at[chunk(j), :]

    def down(k, j):
        return to("pts", fresh(k, j), fresh(k, j), down_send.at[k, j], down_recv.at[k, j], pair)

    def x_copy(o, j):
        return to("cb", block(c, j), block(c, j), x_send.at[o, j], x_recv.at[o, j],
                  ((cx + o) % nx) * CORES + cc)

    def d_copy(o, j):
        ref = block(((cx + nx - o) % nx) * CORES + cc, j)
        return to("cb", ref, ref, d_send.at[o, j], d_recv.at[o, j], sibling)

    def spread(k, j):
        if k == 0:
            for o in range(1, nx):
                x_copy(o, j).start()
            d_copy(0, j).start()

    def min_copy(d):
        return to("cb", mins, mins_in.at[d], min_send.at[d], min_recv.at[d], (c + d) % ncb)

    def tot_copy(d):
        return to("pts", tot, tot_in.at[p], tot_send.at[d], tot_recv.at[d], (p + d) % npts)

    def eye():
        return (lax.broadcasted_iota(jnp.int32, (SPAN, SPAN), 0)
                == lax.broadcasted_iota(jnp.int32, (SPAN, SPAN), 1))

    def lanes(col):
        return jnp.sum(jnp.where(eye(), col, 0.0), axis=0, keepdims=True)

    def upright(row):
        return jnp.sum(jnp.where(eye(), row, 0.0), axis=1, keepdims=True)

    def scale_of(high):
        power = jnp.floor(jnp.log2(TOP / jnp.maximum(high, TINY))).astype(jnp.int32)
        power = jnp.clip(power - LOWEST, 0, 2 ** BITS - 1)
        ratio = jnp.full(high.shape, 2.0 ** LOWEST, F32)
        unit = jnp.full(high.shape, 2.0 ** -LOWEST, F32)
        for bit in range(BITS):
            on = (power // 2 ** bit) % 2 == 1
            ratio = ratio * jnp.where(on, 2.0 ** (2 ** bit), 1.0)
            unit = unit * jnp.where(on, 2.0 ** -(2 ** bit), 1.0)
        return ratio, unit

    def code16(values, ratio):
        return jnp.round(values * ratio).astype(jnp.int32).astype(I16)

    def wide(codes, unit):
        return codes.astype(jnp.int32).astype(F32) * unit

    def pieces_of_sums(k, data, code):
        def one(t, carry):
            with jax.named_scope("sums"):
                label = c * rows + t * SPAN + lax.broadcasted_iota(jnp.int32, (SPAN, npoints), 0)
                hot = jnp.where(code[...] == label, 1.0, 0.0)
                at = span(t * SPAN, SPAN)
                part = jnp.dot(hot.astype(BF16), data[...], preferred_element_type=F32)
                sums[at, :] = part
                ones[0, t] = lanes(jnp.max(jnp.abs(part), axis=1, keepdims=True))
                ones[1, t] = lanes(jnp.sum(hot, axis=1, keepdims=True))

            if k == 0:
                @pl.when(t == 0)
                def _():
                    with jax.named_scope("barrier"):
                        pl.semaphore_wait(barrier, npts - 1 + ncb - 1)

            @pl.when(outer)
            def _():
                with jax.named_scope("quant"):
                    ratio, unit = scale_of(ones[0, t])
                    meta[k, side, t, 0:1, :] = ones[0, t]
                    meta[k, side, t, 1:2, :] = ones[1, t]
                    meta[k, side, t, 2:3, :] = unit
                    meta_up(k, t).start()
                    quant[k, side, at, :] = code16(sums[at, :], upright(ratio))
                    for jj in range(per):
                        up(k, t * per + jj).start()

            return carry

        lax.fori_loop(0, rows // SPAN, one, 0)

    @jax.named_scope("join")
    def join(k, j):
        t = j // per

        @pl.when(j % per == 0)
        def _():
            meta_up(k, t).wait_recv()
            at = span(t * SPAN, SPAN)
            ratio, unit = scale_of(meta_in[k, t, 0:1, :] + ones[0, t])
            meta[k, side, t, 1:2, :] = meta_in[k, t, 1:2, :] + ones[1, t]
            meta[k, side, t, 2:3, :] = unit
            meta_swap(k, t).start()
            cols[0, at, :] = upright(meta_in[k, t, 2:3, :])
            cols[1, at, :] = upright(ratio)

        with jax.named_scope("join_wait"):
            up(k, j).wait_recv()
        at = chunk(j)
        both = sums[at, :] + wide(quant_in[k, at, :], cols[0, at, :])
        quant[k, side, at, :] = code16(both, cols[1, at, :])
        swap(k, j).start()

    @jax.named_scope("settle")
    def settle(k, j, cents):
        t = j // per

        @pl.when(j % per == 0)
        def _():
            meta_swap(k, t).wait_recv()
            at = span(t * SPAN, SPAN)
            share = 1.0 / (meta[k, 0, t, 1:2, :] + meta[k, 1, t, 1:2, :] + 1.0)
            cols[2, at, :] = upright(meta[k, 0, t, 2:3, :])
            cols[3, at, :] = upright(meta[k, 1, t, 2:3, :])
            cols[4, at, :] = upright(share)

        with jax.named_scope("settle_wait"):
            swap(k, j).wait_recv()
        at = chunk(j)
        low = wide(quant[k, 0, at, :], cols[2, at, :])
        high = wide(quant[k, 1, at, :], cols[3, at, :])
        old = cents[at, :].astype(F32)
        fresh(k, j)[...] = ((low + high + old) * cols[4, at, :]).astype(BF16)
        down(k, j).start()
        spread(k, j)

    step = npoints // PIECES

    @jax.named_scope("near_start")
    def near_start(cents):
        cent = cents[...]
        csq[...] = jnp.sum(jnp.square(cent.astype(F32)), axis=1, keepdims=True)
        scaled[...] = (cent * (-2.0)).astype(BF16)
        squares[...] = jnp.zeros(squares.shape, F32)

    @jax.named_scope("near")
    def near_piece(k, data, i):
        at = span(i * step, step)
        rows_in = data[at, :]
        cross = lax.dot_general(scaled[...], rows_in, (((1,), (1,)), ((), ())),
                                preferred_element_type=F32)
        mins[k, :, at] = jnp.min(cross + csq[...], axis=0, keepdims=True)
        sq = jnp.square(rows_in.astype(F32))
        squares[...] += jnp.sum(sq.reshape(step // 8, 8, width), axis=0)

    tile = 128
    setups = 4

    @jax.named_scope("setup")
    def setup(i):
        for j in range(npoints // (tile * setups)):
            at = span(i * (npoints // setups) + j * tile, tile)
            column[at, :] = jnp.broadcast_to(code_one[:, at], (tile, tile)).T
        at = span(i * (npoints // setups), npoints // setups)
        residual[at, :] = points[at, :]

    halves = GROUP // SIZE
    depth = GROUP * ncb
    look_step = 1024

    @jax.named_scope("look")
    def look(b, h):
        @pl.when(h == 0)
        def _():
            for jj in range(halves):
                for o in range(nx):
                    with jax.named_scope("d_wait"):
                        d_copy(o, b * halves + jj).wait_recv()

        labels = []
        for q in range(depth // tile):
            lane = q * tile + lax.broadcasted_iota(jnp.int32, (look_step, tile), 1)
            labels.append((lane // GROUP) * rows + lane % GROUP + b * GROUP)

        def one(s, carry):
            at = span(h * (npoints // halves) + s * look_step, look_step)
            held = column[at, :]
            hot = jnp.concatenate(
                [jnp.where(held == label, 1.0, 0.0).astype(BF16) for label in labels], axis=1
            )
            found = jnp.dot(hot, codebook[span(b * depth, depth), :], preferred_element_type=F32)
            residual[at, :] = (residual[at, :].astype(F32) - found).astype(BF16)
            return carry

        lax.fori_loop(0, npoints // (halves * look_step), one, 0)

    @jax.named_scope("totals")
    def totals():
        for d in range(1, ncb):
            min_copy(d).wait()
        best = mins[...]
        for d in range(1, ncb):
            best = jnp.minimum(best, mins_in[d])
        squares_two = jnp.sum(squares[...], keepdims=True)
        for k in range(2):
            sq = squares_two if k == 1 else tot[0, :, :1]
            tot[k] = jnp.broadcast_to(jnp.sum(best[k], keepdims=True) + sq, tot.shape[1:])
        for d in range(1, npts):
            tot_copy(d).start()

    def exchange(k, data, cents):
        lag_join = HOP
        lag_settle = 2 * HOP
        lag_down = 3 * HOP
        lag_x = jnp.where(inner, 3 * HOP, 4 * HOP)

        def run(i, carry):
            @pl.when(inner)
            def _():
                j = i - lag_settle

                @pl.when(jnp.logical_and(j >= 0, j < n))
                def _():
                    settle(k, j, cents)

                j = i - lag_join

                @pl.when(jnp.logical_and(j >= 0, j < n))
                def _():
                    join(k, j)

            @pl.when(outer)
            def _():
                j = i - lag_down

                @pl.when(jnp.logical_and(j >= 0, j < n))
                def _():
                    with jax.named_scope("down_wait"):
                        down(k, j).wait_recv()
                    spread(k, j)

            @pl.when(i < PIECES)
            def _():
                near_piece(k, data, i)

            if k == 0:
                @pl.when(jnp.logical_and(i >= PIECES, i < PIECES + setups))
                def _():
                    setup(i - PIECES)

                j = i - lag_x

                @pl.when(jnp.logical_and(j >= 0, j < n))
                def _():
                    for o in range(1, nx):
                        with jax.named_scope("x_wait"):
                            x_copy(o, j).wait_recv()
                        d_copy(o, j).start()

                v = i - lag_x - halves - 1

                @pl.when(jnp.logical_and(v >= 0, v < n))
                def _():
                    look(v // halves, v % halves)
            else:
                @pl.when(i == PIECES)
                def _():
                    for d in range(1, ncb):
                        min_copy(d).start()

                @pl.when(i == PIECES + 2 * HOP)
                def _():
                    totals()

            return carry

        steps = n + 4 * HOP + halves + 1 if k == 0 else n + 3 * HOP
        lax.fori_loop(0, steps, run, 0)

    pieces_of_sums(0, points, code_one)
    near_start(cent_one)
    exchange(0, points, cent_one)
    tot[0] = jnp.broadcast_to(jnp.sum(squares[...], keepdims=True), tot.shape[1:])
    pieces_of_sums(1, residual, code_two)
    near_start(cent_two)
    for g in range(rows // GROUP):
        new_one[g * GROUP:(g + 1) * GROUP, :] = codebook[span(g * depth + c * GROUP, GROUP), :]
    exchange(1, residual, cent_two)

    def drain(j, carry):
        for k in range(2):
            @pl.when(outer)
            def _():
                up(k, j).wait_send()

            @pl.when(inner)
            def _():
                swap(k, j).wait_send()
                down(k, j).wait_send()
        for o in range(nx):
            d_copy(o, j).wait_send()
            if o > 0:
                x_copy(o, j).wait_send()
        return carry

    lax.fori_loop(0, n, drain, 0)
    for k in range(2):
        for t in range(rows // SPAN):
            @pl.when(outer)
            def _():
                meta_up(k, t).wait_send()

            @pl.when(inner)
            def _():
                meta_swap(k, t).wait_send()
    for d in range(1, npts):
        tot_copy(d).wait()
    tot_in[p] = tot[...]
    total = tot_in[0]
    for d in range(1, npts):
        total = total + tot_in[d]
    total_out[...] = total / F32(npoints * npts * width)


def fused(points, code_one, code_two, cent_one, cent_two):
    npts = lax.axis_size("pts")
    ncb = lax.axis_size("cb")
    npoints, width = points.shape
    rows = cent_one.shape[0]
    nx = ncb // CORES
    n = rows // SIZE
    spans = rows // SPAN
    vmem = pl.BlockSpec(memory_space=pltpu.VMEM)
    dma = pltpu.SemaphoreType.DMA
    new_one, new_two, total = pl.pallas_call(
        functools.partial(fused_kernel, npts, ncb),
        out_shape=(
            jax.ShapeDtypeStruct(cent_one.shape, BF16),
            jax.ShapeDtypeStruct(cent_two.shape, BF16),
            jax.ShapeDtypeStruct((2, 1, 128), F32),
        ),
        in_specs=[vmem] * 5,
        out_specs=(vmem,) * 3,
        scratch_shapes=[
            pltpu.VMEM(points.shape, BF16),
            pltpu.VMEM((rows * ncb, width), BF16),
            pltpu.VMEM((rows, width), F32),
            pltpu.VMEM((2, 2, rows, width), I16),
            pltpu.VMEM((2, rows, width), I16),
            pltpu.VMEM((2, 2, spans, 4, SPAN), F32),
            pltpu.VMEM((2, spans, 4, SPAN), F32),
            pltpu.VMEM((5, rows, 1), F32),
            pltpu.VMEM((2, spans, 1, SPAN), F32),
            pltpu.VMEM((npoints, 128), jnp.int32),
            pltpu.VMEM((2, 1, npoints), F32),
            pltpu.VMEM((ncb, 2, 1, npoints), F32),
            pltpu.VMEM((2, 1, 128), F32),
            pltpu.VMEM((npts, 2, 1, 128), F32),
            pltpu.VMEM((rows, width), BF16),
            pltpu.VMEM((rows, 1), F32),
            pltpu.VMEM((8, width), F32),
            dma((2, n)), dma((2, n)), dma((2, n)), dma((2, n)), dma((2, n)), dma((2, n)),
            dma((2, spans)), dma((2, spans)), dma((2, spans)), dma((2, spans)),
            dma((nx, n)), dma((nx, n)), dma((nx, n)), dma((nx, n)),
            dma((ncb,)), dma((ncb,)), dma((npts,)), dma((npts,)),
        ],
        compiler_params=pltpu.CompilerParams(
            collective_id=0, has_side_effects=True, vmem_limit_bytes=60 * 1024 * 1024
        ),
    )(points, code_one.reshape(1, npoints), code_two.reshape(1, npoints), cent_one, cent_two)
    return new_one, new_two, total[:, 0, 0]


def nearest_local(data, cents):
    sq = jnp.sum(jnp.square(data.astype(jnp.float32)), axis=1)
    csq = jnp.sum(jnp.square(cents.astype(jnp.float32)), axis=1)
    cross = lax.dot_general(
        data, cents, (((1,), (1,)), ((), ())), preferred_element_type=jnp.float32
    )
    dist = sq[:, None] - 2.0 * cross + csq[None, :]
    local_min = jnp.min(dist, axis=1)
    best = lax.pmin(local_min, "cb")
    return jnp.sum(best)


def section_update(data, codes, cents):
    rows = cents.shape[0]
    first = lax.axis_index("cb") * rows
    labels = first + lax.broadcasted_iota(jnp.int32, (1, rows), 1)
    onehot = (codes[:, None] == labels).astype(jnp.bfloat16)
    sums = lax.dot_general(
        onehot, data, (((0,), (0,)), ((), ())), preferred_element_type=jnp.float32
    )
    counts = jnp.sum(onehot.astype(jnp.float32), axis=0)
    share_sums, share_counts = (
        lax.psum_scatter(sums, "pts", scatter_dimension=0, tiled=True),
        lax.psum_scatter(counts, "pts", scatter_dimension=0, tiled=True),
    )
    share_rows = share_sums.shape[0]
    old_rows = lax.dynamic_slice_in_dim(cents, lax.axis_index("pts") * share_rows, share_rows, 0)
    return ((share_sums + old_rows.astype(jnp.float32)) / (share_counts + 1.0)[:, None]).astype(
        jnp.bfloat16
    )


def section_total(value):
    return lax.psum(value, "pts")


def local(points, code_one, code_two, cent_one, cent_two):
    rows = cent_one.shape[0]
    width = points.shape[1]
    npts = lax.axis_size("pts")
    ncb = lax.axis_size("cb")
    first = lax.axis_index("cb") * rows
    first_local = nearest_local(points, cent_one)
    updated_one = section_update(points, code_one, cent_one)
    gathered = lax.all_gather(updated_one, ("pts", "cb"), axis=0, tiled=True)
    share_rows = updated_one.shape[0]
    codebook = jnp.swapaxes(gathered.reshape(npts, ncb, share_rows, width), 0, 1).reshape(
        rows * ncb, width
    )
    new_one = lax.dynamic_slice_in_dim(codebook, first, rows, 0)
    looked = jnp.take(codebook, code_one, axis=0)
    residual = (points.astype(jnp.float32) - looked.astype(jnp.float32)).astype(jnp.bfloat16)
    updated_two = section_update(residual, code_two, cent_two)
    new_two = lax.all_gather(updated_two, "pts", axis=0, tiled=True)
    second_local = nearest_local(residual, cent_two)
    first_sum = section_total(first_local)
    second_sum = section_total(second_local)
    scale = jnp.float32(points.shape[0] * npts * width)
    distortion = jnp.stack([first_sum, second_sum]) / scale
    return (new_one, new_two, distortion)


def choose(points, code_one, code_two, cent_one, cent_two):
    rows, npts, ncb = cent_one.shape[0], lax.axis_size("pts"), lax.axis_size("cb")
    fits = (
        npts == 4
        and ncb % CORES == 0
        and (ncb * GROUP) % 128 == 0
        and rows % SPAN == 0
        and points.shape[0] % 2048 == 0
    )
    form = fused if fits else local
    return form(points, code_one, code_two, cent_one, cent_two)


def solution(mesh):
    return jax.shard_map(
        choose,
        mesh=mesh,
        in_specs=(
            P(("groups", "pts"), None),
            P(("groups", "pts")),
            P(("groups", "pts")),
            P(("groups", "cb"), None),
            P(("groups", "cb"), None),
        ),
        out_specs=(P(("groups", "cb"), None), P(("groups", "cb"), None), P("groups")),
        check_vma=False,
    )
```

```python
import functools

import jax
import jax.numpy as jnp
from jax import lax
from jax.experimental import pallas as pl
from jax.experimental.pallas import tpu as pltpu
from jax.sharding import PartitionSpec as P

F32 = jnp.float32
BF16 = jnp.bfloat16
I16 = jnp.int16
CORES = 2
SIZE = 32
SPAN = 128
GROUP = 64
PIECES = 8
LJ = 3
LS = 7
LD = 11
LX = 4
LK = 3
TOP = 32700.0
TINY = 2.0 ** -100
LOWEST = -16
BITS = 7


def fused_kernel(
    npts, ncb,
    points_in, code_one_in, code_two_in, cent_one_in, cent_two_in,
    new_one, new_two, total_out,
    points, code_one, code_two, cent_one, cent_two, load_sem,
    residual, codebook, sums, quant, quant_in, meta, meta_in, cols, ones, column,
    mins, mins_in, tot, tot_in, scaled, csq, squares,
    up_send, up_recv, swap_send, swap_recv, down_send, down_recv,
    mup_send, mup_recv, mswap_send, mswap_recv,
    x_send, x_recv, d_send, d_recv, min_send, min_recv, tot_send, tot_recv,
):
    loads = [
        pltpu.make_async_copy(src, dst, load_sem.at[at])
        for at, (src, dst) in enumerate((
            (code_one_in, code_one), (points_in, points), (cent_one_in, cent_one),
            (code_two_in, code_two), (cent_two_in, cent_two),
        ))
    ]
    for load in loads:
        load.start()
    p = lax.axis_index("pts")
    c = lax.axis_index("cb")
    npoints, width = points.shape
    rows = cent_one.shape[0]
    n = rows // SIZE
    per = SPAN // SIZE
    nx = ncb // CORES
    cx, cc = c // CORES, c % CORES
    sibling = cx * CORES + (1 - cc)
    side = p // 2
    inner = jnp.logical_or(p == 1, p == 2)
    outer = jnp.logical_not(inner)
    pair = p + 1 - 2 * (p % 2)
    across = npts - 1 - p

    def to(axis, src, dst, s, r, where):
        return pltpu.make_async_remote_copy(
            src_ref=src, dst_ref=dst, send_sem=s, recv_sem=r,
            device_id={axis: where}, device_id_type=pl.DeviceIdType.MESH,
        )

    barrier = pltpu.get_barrier_semaphore()
    for d in range(1, npts):
        pl.semaphore_signal(barrier, inc=1, device_id={"pts": (p + d) % npts},
                            device_id_type=pl.DeviceIdType.MESH)
    for d in range(1, ncb):
        pl.semaphore_signal(barrier, inc=1, device_id={"cb": (c + d) % ncb},
                            device_id_type=pl.DeviceIdType.MESH)

    def span(start, length):
        return pl.ds(pl.multiple_of(start, length), length)

    def chunk(j):
        return span(j * SIZE, SIZE)

    def up(k, j):
        return to("pts", quant.at[k, side, chunk(j), :], quant_in.at[k, chunk(j), :],
                  up_send.at[k, j], up_recv.at[k, j], pair)

    def swap(k, j):
        ref = quant.at[k, side, chunk(j), :]
        return to("pts", ref, ref, swap_send.at[k, j], swap_recv.at[k, j], across)

    def meta_up(k, t):
        return to("pts", meta.at[k, side, t], meta_in.at[k, t], mup_send.at[k, t],
                  mup_recv.at[k, t], pair)

    def meta_swap(k, t):
        ref = meta.at[k, side, t]
        return to("pts", ref, ref, mswap_send.at[k, t], mswap_recv.at[k, t], across)

    def block(col, j):
        first = j * SIZE
        at = (first // GROUP) * (GROUP * ncb) + col * GROUP + first % GROUP
        return codebook.at[span(at, SIZE), :]

    def fresh(k, j):
        return block(c, j) if k == 0 else new_two.at[chunk(j), :]

    def down(k, j):
        return to("pts", fresh(k, j), fresh(k, j), down_send.at[k, j], down_recv.at[k, j], pair)

    def x_copy(o, j):
        return to("cb", block(c, j), block(c, j), x_send.at[o, j], x_recv.at[o, j],
                  ((cx + o) % nx) * CORES + cc)

    def d_copy(o, j):
        ref = block(((cx + nx - o) % nx) * CORES + cc, j)
        return to("cb", ref, ref, d_send.at[o, j], d_recv.at[o, j], sibling)

    def spread(k, j):
        if k == 0:
            for o in range(1, nx):
                x_copy(o, j).start()
            d_copy(0, j).start()

    def min_copy(d):
        return to("cb", mins, mins_in.at[d], min_send.at[d], min_recv.at[d], (c + d) % ncb)

    def tot_copy(d):
        return to("pts", tot, tot_in.at[p], tot_send.at[d], tot_recv.at[d], (p + d) % npts)

    def eye():
        return (lax.broadcasted_iota(jnp.int32, (SPAN, SPAN), 0)
                == lax.broadcasted_iota(jnp.int32, (SPAN, SPAN), 1))

    def lanes(col):
        return jnp.sum(jnp.where(eye(), col, 0.0), axis=0, keepdims=True)

    def upright(row):
        return jnp.sum(jnp.where(eye(), row, 0.0), axis=1, keepdims=True)

    def scale_of(high):
        power = jnp.floor(jnp.log2(TOP / jnp.maximum(high, TINY))).astype(jnp.int32)
        power = jnp.clip(power - LOWEST, 0, 2 ** BITS - 1)
        ratio = jnp.full(high.shape, 2.0 ** LOWEST, F32)
        unit = jnp.full(high.shape, 2.0 ** -LOWEST, F32)
        for bit in range(BITS):
            on = (power // 2 ** bit) % 2 == 1
            ratio = ratio * jnp.where(on, 2.0 ** (2 ** bit), 1.0)
            unit = unit * jnp.where(on, 2.0 ** -(2 ** bit), 1.0)
        return ratio, unit

    def code16(values, ratio):
        return jnp.round(values * ratio).astype(jnp.int32).astype(I16)

    def wide(codes, unit):
        return codes.astype(jnp.int32).astype(F32) * unit

    def pieces_of_sums(k, data, code):
        def one(t, carry):
            with jax.named_scope("sums"):
                label = c * rows + t * SPAN + lax.broadcasted_iota(jnp.int32, (SPAN, npoints), 0)
                hot = jnp.where(code[...] == label, 1.0, 0.0)
                at = span(t * SPAN, SPAN)
                part = jnp.dot(hot.astype(BF16), data[...], preferred_element_type=F32)
                sums[at, :] = part
                ones[0, t] = lanes(jnp.max(jnp.abs(part), axis=1, keepdims=True))
                ones[1, t] = lanes(jnp.sum(hot, axis=1, keepdims=True))

            if k == 0:
                @pl.when(t == 0)
                def _():
                    with jax.named_scope("barrier"):
                        pl.semaphore_wait(barrier, npts - 1 + ncb - 1)

            @pl.when(outer)
            def _():
                with jax.named_scope("quant"):
                    ratio, unit = scale_of(ones[0, t])
                    meta[k, side, t, 0:1, :] = ones[0, t]
                    meta[k, side, t, 1:2, :] = ones[1, t]
                    meta[k, side, t, 2:3, :] = unit
                    meta_up(k, t).start()
                    quant[k, side, at, :] = code16(sums[at, :], upright(ratio))
                    for jj in range(per):
                        up(k, t * per + jj).start()

            return carry

        lax.fori_loop(0, rows // SPAN, one, 0)

    @jax.named_scope("join")
    def join(k, j):
        t = j // per

        @pl.when(j % per == 0)
        def _():
            meta_up(k, t).wait_recv()
            at = span(t * SPAN, SPAN)
            ratio, unit = scale_of(meta_in[k, t, 0:1, :] + ones[0, t])
            meta[k, side, t, 1:2, :] = meta_in[k, t, 1:2, :] + ones[1, t]
            meta[k, side, t, 2:3, :] = unit
            meta_swap(k, t).start()
            cols[0, at, :] = upright(meta_in[k, t, 2:3, :])
            cols[1, at, :] = upright(ratio)

        with jax.named_scope("join_wait"):
            up(k, j).wait_recv()
        at = chunk(j)
        both = sums[at, :] + wide(quant_in[k, at, :], cols[0, at, :])
        quant[k, side, at, :] = code16(both, cols[1, at, :])
        swap(k, j).start()

    @jax.named_scope("settle")
    def settle(k, j, cents):
        t = j // per

        @pl.when(j % per == 0)
        def _():
            meta_swap(k, t).wait_recv()
            at = span(t * SPAN, SPAN)
            share = 1.0 / (meta[k, 0, t, 1:2, :] + meta[k, 1, t, 1:2, :] + 1.0)
            cols[2, at, :] = upright(meta[k, 0, t, 2:3, :])
            cols[3, at, :] = upright(meta[k, 1, t, 2:3, :])
            cols[4, at, :] = upright(share)

        with jax.named_scope("settle_wait"):
            swap(k, j).wait_recv()
        at = chunk(j)
        low = wide(quant[k, 0, at, :], cols[2, at, :])
        high = wide(quant[k, 1, at, :], cols[3, at, :])
        old = cents[at, :].astype(F32)
        fresh(k, j)[...] = ((low + high + old) * cols[4, at, :]).astype(BF16)
        down(k, j).start()
        spread(k, j)

    step = npoints // PIECES

    @jax.named_scope("near_start")
    def near_start(cents):
        cent = cents[...]
        csq[...] = jnp.sum(jnp.square(cent.astype(F32)), axis=1, keepdims=True)
        scaled[...] = (cent * (-2.0)).astype(BF16)
        squares[...] = jnp.zeros(squares.shape, F32)

    @jax.named_scope("near")
    def near_piece(k, data, i):
        at = span(i * step, step)
        rows_in = data[at, :]
        cross = lax.dot_general(scaled[...], rows_in, (((1,), (1,)), ((), ())),
                                preferred_element_type=F32)
        mins[k, :, at] = jnp.min(cross + csq[...], axis=0, keepdims=True)
        sq = jnp.square(rows_in.astype(F32))
        squares[...] += jnp.sum(sq.reshape(step // 8, 8, width), axis=0)

    tile = 128
    setups = 4

    @jax.named_scope("setup")
    def setup(i):
        for j in range(npoints // (tile * setups)):
            at = span(i * (npoints // setups) + j * tile, tile)
            column[at, :] = jnp.broadcast_to(code_one[:, at], (tile, tile)).T
        at = span(i * (npoints // setups), npoints // setups)
        residual[at, :] = points[at, :]

    halves = GROUP // SIZE
    looks = 2
    depth = GROUP * ncb
    look_step = 1024

    @jax.named_scope("look")
    def look(b, h):
        @pl.when(h == 0)
        def _():
            for jj in range(halves):
                for o in range(nx):
                    with jax.named_scope("d_wait"):
                        d_copy(o, b * halves + jj).wait_recv()

        labels = []
        for q in range(depth // tile):
            lane = q * tile + lax.broadcasted_iota(jnp.int32, (look_step, tile), 1)
            labels.append((lane // GROUP) * rows + lane % GROUP + b * GROUP)

        def one(s, carry):
            at = span(h * (npoints // looks) + s * look_step, look_step)
            held = column[at, :]
            hot = jnp.concatenate(
                [jnp.where(held == label, 1.0, 0.0).astype(BF16) for label in labels], axis=1
            )
            found = jnp.dot(hot, codebook[span(b * depth, depth), :], preferred_element_type=F32)
            residual[at, :] = (residual[at, :].astype(F32) - found).astype(BF16)
            return carry

        lax.fori_loop(0, npoints // (looks * look_step), one, 0)

    @jax.named_scope("totals")
    def totals():
        for d in range(1, ncb):
            min_copy(d).wait()
        best = mins[...]
        for d in range(1, ncb):
            best = jnp.minimum(best, mins_in[d])
        squares_two = jnp.sum(squares[...], keepdims=True)
        for k in range(2):
            sq = squares_two if k == 1 else tot[0, :, :1]
            tot[k] = jnp.broadcast_to(jnp.sum(best[k], keepdims=True) + sq, tot.shape[1:])
        for d in range(1, npts):
            tot_copy(d).start()

    def exchange(k, data, cents):
        lag_join = LJ
        lag_settle = LS
        lag_down = LD
        lag_x = jnp.where(inner, LS, LD) + LX

        def run(i, carry):
            @pl.when(inner)
            def _():
                j = i - lag_settle

                @pl.when(jnp.logical_and(j >= 0, j < n))
                def _():
                    settle(k, j, cents)

                j = i - lag_join

                @pl.when(jnp.logical_and(j >= 0, j < n))
                def _():
                    join(k, j)

            @pl.when(outer)
            def _():
                j = i - lag_down

                @pl.when(jnp.logical_and(j >= 0, j < n))
                def _():
                    with jax.named_scope("down_wait"):
                        down(k, j).wait_recv()
                    spread(k, j)

            @pl.when(i < PIECES)
            def _():
                near_piece(k, data, i)

            if k == 0:
                @pl.when(jnp.logical_and(i >= PIECES, i < PIECES + setups))
                def _():
                    setup(i - PIECES)

                j = i - lag_x

                @pl.when(jnp.logical_and(j >= 0, j < n))
                def _():
                    for o in range(1, nx):
                        with jax.named_scope("x_wait"):
                            x_copy(o, j).wait_recv()
                        d_copy(o, j).start()

                v = i - lag_x - LK

                every = halves // looks

                @pl.when(jnp.logical_and(v >= 0, jnp.logical_and(v < n, v % every == 0)))
                def _():
                    look(v // halves, (v % halves) // every)
            else:
                @pl.when(i == PIECES)
                def _():
                    for d in range(1, ncb):
                        min_copy(d).start()

                @pl.when(i == PIECES + 6)
                def _():
                    totals()

            return carry

        steps = n + LD + LX + LK if k == 0 else n + LD
        lax.fori_loop(0, steps, run, 0)

    loads[0].wait()
    loads[1].wait()
    pieces_of_sums(0, points, code_one)
    loads[2].wait()
    loads[3].wait()
    loads[4].wait()
    near_start(cent_one)
    exchange(0, points, cent_one)
    tot[0] = jnp.broadcast_to(jnp.sum(squares[...], keepdims=True), tot.shape[1:])
    pieces_of_sums(1, residual, code_two)
    near_start(cent_two)
    for g in range(rows // GROUP):
        new_one[g * GROUP:(g + 1) * GROUP, :] = codebook[span(g * depth + c * GROUP, GROUP), :]
    exchange(1, residual, cent_two)

    def drain(j, carry):
        for k in range(2):
            @pl.when(outer)
            def _():
                up(k, j).wait_send()

            @pl.when(inner)
            def _():
                swap(k, j).wait_send()
                down(k, j).wait_send()
        for o in range(nx):
            d_copy(o, j).wait_send()
            if o > 0:
                x_copy(o, j).wait_send()
        return carry

    lax.fori_loop(0, n, drain, 0)
    for k in range(2):
        for t in range(rows // SPAN):
            @pl.when(outer)
            def _():
                meta_up(k, t).wait_send()

            @pl.when(inner)
            def _():
                meta_swap(k, t).wait_send()
    for d in range(1, npts):
        tot_copy(d).wait()
    tot_in[p] = tot[...]
    total = tot_in[0]
    for d in range(1, npts):
        total = total + tot_in[d]
    total_out[...] = total / F32(npoints * npts * width)


def finish_kernel(one_in, two_in, total_in, one_out, two_out, total_out, sem):
    first = pltpu.make_async_copy(one_in, one_out, sem.at[0])
    second = pltpu.make_async_copy(two_in, two_out, sem.at[1])
    first.start()
    second.start()
    for k in range(2):
        total_out[k] = jnp.sum(total_in[k, :, :1])
    first.wait()
    second.wait()


def finish(new_one, new_two, total):
    vmem = pl.BlockSpec(memory_space=pltpu.VMEM)
    anywhere = pl.BlockSpec(memory_space=pl.ANY)
    return pl.pallas_call(
        finish_kernel,
        out_shape=(
            jax.ShapeDtypeStruct(new_one.shape, BF16),
            jax.ShapeDtypeStruct(new_two.shape, BF16),
            jax.ShapeDtypeStruct((2,), F32),
        ),
        in_specs=[vmem] * 3,
        out_specs=(anywhere, anywhere, pl.BlockSpec(memory_space=pltpu.SMEM)),
        scratch_shapes=[pltpu.SemaphoreType.DMA((2,))],
        compiler_params=pltpu.CompilerParams(vmem_limit_bytes=8 * 1024 * 1024),
    )(new_one, new_two, total)


def fused(points, code_one, code_two, cent_one, cent_two):
    npts = lax.axis_size("pts")
    ncb = lax.axis_size("cb")
    npoints, width = points.shape
    rows = cent_one.shape[0]
    nx = ncb // CORES
    n = rows // SIZE
    spans = rows // SPAN
    vmem = pl.BlockSpec(memory_space=pltpu.VMEM)
    dma = pltpu.SemaphoreType.DMA
    new_one, new_two, total = pl.pallas_call(
        functools.partial(fused_kernel, npts, ncb),
        out_shape=(
            pltpu.VMEM(cent_one.shape, BF16),
            pltpu.VMEM(cent_two.shape, BF16),
            pltpu.VMEM((2, 1, 128), F32),
        ),
        in_specs=[pl.BlockSpec(memory_space=pl.ANY)] * 5,
        out_specs=(vmem,) * 3,
        scratch_shapes=[
            pltpu.VMEM(points.shape, BF16),
            pltpu.VMEM((1, npoints), jnp.int32),
            pltpu.VMEM((1, npoints), jnp.int32),
            pltpu.VMEM(cent_one.shape, BF16),
            pltpu.VMEM(cent_two.shape, BF16),
            dma((5,)),
            pltpu.VMEM(points.shape, BF16),
            pltpu.VMEM((rows * ncb, width), BF16),
            pltpu.VMEM((rows, width), F32),
            pltpu.VMEM((2, 2, rows, width), I16),
            pltpu.VMEM((2, rows, width), I16),
            pltpu.VMEM((2, 2, spans, 4, SPAN), F32),
            pltpu.VMEM((2, spans, 4, SPAN), F32),
            pltpu.VMEM((5, rows, 1), F32),
            pltpu.VMEM((2, spans, 1, SPAN), F32),
            pltpu.VMEM((npoints, 128), jnp.int32),
            pltpu.VMEM((2, 1, npoints), F32),
            pltpu.VMEM((ncb, 2, 1, npoints), F32),
            pltpu.VMEM((2, 1, 128), F32),
            pltpu.VMEM((npts, 2, 1, 128), F32),
            pltpu.VMEM((rows, width), BF16),
            pltpu.VMEM((rows, 1), F32),
            pltpu.VMEM((8, width), F32),
            dma((2, n)), dma((2, n)), dma((2, n)), dma((2, n)), dma((2, n)), dma((2, n)),
            dma((2, spans)), dma((2, spans)), dma((2, spans)), dma((2, spans)),
            dma((nx, n)), dma((nx, n)), dma((nx, n)), dma((nx, n)),
            dma((ncb,)), dma((ncb,)), dma((npts,)), dma((npts,)),
        ],
        compiler_params=pltpu.CompilerParams(
            collective_id=0, has_side_effects=True, vmem_limit_bytes=60 * 1024 * 1024
        ),
    )(points, code_one.reshape(1, npoints), code_two.reshape(1, npoints), cent_one, cent_two)
    return finish(new_one, new_two, total)


def nearest_local(data, cents):
    sq = jnp.sum(jnp.square(data.astype(jnp.float32)), axis=1)
    csq = jnp.sum(jnp.square(cents.astype(jnp.float32)), axis=1)
    cross = lax.dot_general(
        data, cents, (((1,), (1,)), ((), ())), preferred_element_type=jnp.float32
    )
    dist = sq[:, None] - 2.0 * cross + csq[None, :]
    local_min = jnp.min(dist, axis=1)
    best = lax.pmin(local_min, "cb")
    return jnp.sum(best)


def section_update(data, codes, cents):
    rows = cents.shape[0]
    first = lax.axis_index("cb") * rows
    labels = first + lax.broadcasted_iota(jnp.int32, (1, rows), 1)
    onehot = (codes[:, None] == labels).astype(jnp.bfloat16)
    sums = lax.dot_general(
        onehot, data, (((0,), (0,)), ((), ())), preferred_element_type=jnp.float32
    )
    counts = jnp.sum(onehot.astype(jnp.float32), axis=0)
    share_sums, share_counts = (
        lax.psum_scatter(sums, "pts", scatter_dimension=0, tiled=True),
        lax.psum_scatter(counts, "pts", scatter_dimension=0, tiled=True),
    )
    share_rows = share_sums.shape[0]
    old_rows = lax.dynamic_slice_in_dim(cents, lax.axis_index("pts") * share_rows, share_rows, 0)
    return ((share_sums + old_rows.astype(jnp.float32)) / (share_counts + 1.0)[:, None]).astype(
        jnp.bfloat16
    )


def section_total(value):
    return lax.psum(value, "pts")


def local(points, code_one, code_two, cent_one, cent_two):
    rows = cent_one.shape[0]
    width = points.shape[1]
    npts = lax.axis_size("pts")
    ncb = lax.axis_size("cb")
    first = lax.axis_index("cb") * rows
    first_local = nearest_local(points, cent_one)
    updated_one = section_update(points, code_one, cent_one)
    gathered = lax.all_gather(updated_one, ("pts", "cb"), axis=0, tiled=True)
    share_rows = updated_one.shape[0]
    codebook = jnp.swapaxes(gathered.reshape(npts, ncb, share_rows, width), 0, 1).reshape(
        rows * ncb, width
    )
    new_one = lax.dynamic_slice_in_dim(codebook, first, rows, 0)
    looked = jnp.take(codebook, code_one, axis=0)
    residual = (points.astype(jnp.float32) - looked.astype(jnp.float32)).astype(jnp.bfloat16)
    updated_two = section_update(residual, code_two, cent_two)
    new_two = lax.all_gather(updated_two, "pts", axis=0, tiled=True)
    second_local = nearest_local(residual, cent_two)
    first_sum = section_total(first_local)
    second_sum = section_total(second_local)
    scale = jnp.float32(points.shape[0] * npts * width)
    distortion = jnp.stack([first_sum, second_sum]) / scale
    return (new_one, new_two, distortion)


def choose(points, code_one, code_two, cent_one, cent_two):
    rows, npts, ncb = cent_one.shape[0], lax.axis_size("pts"), lax.axis_size("cb")
    fits = (
        npts == 4
        and ncb % CORES == 0
        and (ncb * GROUP) % 128 == 0
        and rows % SPAN == 0
        and points.shape[0] % 2048 == 0
    )
    form = fused if fits else local
    return form(points, code_one, code_two, cent_one, cent_two)


def solution(mesh):
    return jax.shard_map(
        choose,
        mesh=mesh,
        in_specs=(
            P(("groups", "pts"), None),
            P(("groups", "pts")),
            P(("groups", "pts")),
            P(("groups", "cb"), None),
            P(("groups", "cb"), None),
        ),
        out_specs=(P(("groups", "cb"), None), P(("groups", "cb"), None), P("groups")),
        check_vma=False,
    )
```

```python
import functools

import jax
import jax.numpy as jnp
from jax import lax
from jax.experimental import pallas as pl
from jax.experimental.pallas import tpu as pltpu
from jax.sharding import PartitionSpec as P

F32 = jnp.float32
BF16 = jnp.bfloat16
I16 = jnp.int16
CORES = 2
SIZE = 32
SPAN = 128
GROUP = 64
PIECES = 8
LJ = 3
LS = 7
LD = 11
LX = 4
LK = 3
TOP = 32700.0
TINY = 2.0 ** -100
LOWEST = -16
BITS = 7


def fused_kernel(
    npts, ncb,
    points_in, code_one_in, code_two_in, cent_one_in, cent_two_in,
    new_one, new_two, total_out,
    points, code_one, code_two, cent_one, cent_two, load_sem,
    residual, codebook, sums, quant, quant_in, meta, meta_in, cols, ones, column,
    mins, mins_in, tot, tot_in, scaled, csq, squares,
    up_send, up_recv, swap_send, swap_recv, down_send, down_recv,
    mup_send, mup_recv, mswap_send, mswap_recv,
    x_send, x_recv, d_send, d_recv, min_send, min_recv, tot_send, tot_recv,
):
    loads = [
        pltpu.make_async_copy(src, dst, load_sem.at[at])
        for at, (src, dst) in enumerate((
            (code_one_in, code_one), (points_in, points), (cent_one_in, cent_one),
            (code_two_in, code_two), (cent_two_in, cent_two),
        ))
    ]
    for load in loads:
        load.start()
    p = lax.axis_index("pts")
    c = lax.axis_index("cb")
    npoints, width = points.shape
    rows = cent_one.shape[0]
    n = rows // SIZE
    per = SPAN // SIZE
    nx = ncb // CORES
    cx, cc = c // CORES, c % CORES
    sibling = cx * CORES + (1 - cc)
    side = p // 2
    inner = jnp.logical_or(p == 1, p == 2)
    outer = jnp.logical_not(inner)
    pair = p + 1 - 2 * (p % 2)
    across = npts - 1 - p

    def to(axis, src, dst, s, r, where):
        return pltpu.make_async_remote_copy(
            src_ref=src, dst_ref=dst, send_sem=s, recv_sem=r,
            device_id={axis: where}, device_id_type=pl.DeviceIdType.MESH,
        )

    barrier = pltpu.get_barrier_semaphore()
    for d in range(1, npts):
        pl.semaphore_signal(barrier, inc=1, device_id={"pts": (p + d) % npts},
                            device_id_type=pl.DeviceIdType.MESH)
    for d in range(1, ncb):
        pl.semaphore_signal(barrier, inc=1, device_id={"cb": (c + d) % ncb},
                            device_id_type=pl.DeviceIdType.MESH)

    def span(start, length):
        return pl.ds(pl.multiple_of(start, length), length)

    def chunk(j):
        return span(j * SIZE, SIZE)

    def up(k, j):
        return to("pts", quant.at[k, side, chunk(j), :], quant_in.at[k, chunk(j), :],
                  up_send.at[k, j], up_recv.at[k, j], pair)

    def swap(k, j):
        ref = quant.at[k, side, chunk(j), :]
        return to("pts", ref, ref, swap_send.at[k, j], swap_recv.at[k, j], across)

    def meta_up(k, t):
        return to("pts", meta.at[k, side, t], meta_in.at[k, t], mup_send.at[k, t],
                  mup_recv.at[k, t], pair)

    def meta_swap(k, t):
        ref = meta.at[k, side, t]
        return to("pts", ref, ref, mswap_send.at[k, t], mswap_recv.at[k, t], across)

    def block(col, j):
        first = j * SIZE
        at = (first // GROUP) * (GROUP * ncb) + col * GROUP + first % GROUP
        return codebook.at[span(at, SIZE), :]

    def fresh(k, j):
        return block(c, j) if k == 0 else new_two.at[chunk(j), :]

    def down(k, j):
        return to("pts", fresh(k, j), fresh(k, j), down_send.at[k, j], down_recv.at[k, j], pair)

    def x_copy(o, j):
        return to("cb", block(c, j), block(c, j), x_send.at[o, j], x_recv.at[o, j],
                  ((cx + o) % nx) * CORES + cc)

    def d_copy(o, j):
        ref = block(((cx + nx - o) % nx) * CORES + cc, j)
        return to("cb", ref, ref, d_send.at[o, j], d_recv.at[o, j], sibling)

    def spread(k, j):
        if k == 0:
            for o in range(1, nx):
                x_copy(o, j).start()
            d_copy(0, j).start()

    def min_copy(d):
        return to("cb", mins, mins_in.at[d], min_send.at[d], min_recv.at[d], (c + d) % ncb)

    def tot_copy(d):
        return to("pts", tot, tot_in.at[p], tot_send.at[d], tot_recv.at[d], (p + d) % npts)

    def eye():
        return (lax.broadcasted_iota(jnp.int32, (SPAN, SPAN), 0)
                == lax.broadcasted_iota(jnp.int32, (SPAN, SPAN), 1))

    def lanes(col):
        return jnp.sum(jnp.where(eye(), col, 0.0), axis=0, keepdims=True)

    def upright(row):
        return jnp.sum(jnp.where(eye(), row, 0.0), axis=1, keepdims=True)

    def scale_of(high):
        power = jnp.floor(jnp.log2(TOP / jnp.maximum(high, TINY))).astype(jnp.int32)
        power = jnp.clip(power - LOWEST, 0, 2 ** BITS - 1)
        ratio = jnp.full(high.shape, 2.0 ** LOWEST, F32)
        unit = jnp.full(high.shape, 2.0 ** -LOWEST, F32)
        for bit in range(BITS):
            on = (power // 2 ** bit) % 2 == 1
            ratio = ratio * jnp.where(on, 2.0 ** (2 ** bit), 1.0)
            unit = unit * jnp.where(on, 2.0 ** -(2 ** bit), 1.0)
        return ratio, unit

    def code16(values, ratio):
        return jnp.round(values * ratio).astype(jnp.int32).astype(I16)

    def wide(codes, unit):
        return codes.astype(jnp.int32).astype(F32) * unit

    def pieces_of_sums(k, data, code):
        def one(t, carry):
            with jax.named_scope("sums"):
                label = c * rows + t * SPAN + lax.broadcasted_iota(jnp.int32, (SPAN, npoints), 0)
                hot = jnp.where(code[...] == label, 1.0, 0.0)
                at = span(t * SPAN, SPAN)
                part = jnp.dot(hot.astype(BF16), data[...], preferred_element_type=F32)
                sums[at, :] = part
                ones[0, t] = lanes(jnp.max(jnp.abs(part), axis=1, keepdims=True))
                ones[1, t] = lanes(jnp.sum(hot, axis=1, keepdims=True))

            if k == 0:
                @pl.when(t == 0)
                def _():
                    with jax.named_scope("barrier"):
                        pl.semaphore_wait(barrier, npts - 1 + ncb - 1)

            @pl.when(outer)
            def _():
                with jax.named_scope("quant"):
                    ratio, unit = scale_of(ones[0, t])
                    meta[k, side, t, 0:1, :] = ones[0, t]
                    meta[k, side, t, 1:2, :] = ones[1, t]
                    meta[k, side, t, 2:3, :] = unit
                    meta_up(k, t).start()
                    quant[k, side, at, :] = code16(sums[at, :], upright(ratio))
                    for jj in range(per):
                        up(k, t * per + jj).start()

            return carry

        lax.fori_loop(0, rows // SPAN, one, 0)

    @jax.named_scope("join")
    def join(k, j):
        t = j // per

        @pl.when(j % per == 0)
        def _():
            meta_up(k, t).wait_recv()
            at = span(t * SPAN, SPAN)
            ratio, unit = scale_of(meta_in[k, t, 0:1, :] + ones[0, t])
            meta[k, side, t, 1:2, :] = meta_in[k, t, 1:2, :] + ones[1, t]
            meta[k, side, t, 2:3, :] = unit
            meta_swap(k, t).start()
            cols[0, at, :] = upright(meta_in[k, t, 2:3, :])
            cols[1, at, :] = upright(ratio)

        with jax.named_scope("join_wait"):
            up(k, j).wait_recv()
        at = chunk(j)
        both = sums[at, :] + wide(quant_in[k, at, :], cols[0, at, :])
        quant[k, side, at, :] = code16(both, cols[1, at, :])
        swap(k, j).start()

    @jax.named_scope("settle")
    def settle(k, j, cents):
        t = j // per

        @pl.when(j % per == 0)
        def _():
            meta_swap(k, t).wait_recv()
            at = span(t * SPAN, SPAN)
            share = 1.0 / (meta[k, 0, t, 1:2, :] + meta[k, 1, t, 1:2, :] + 1.0)
            cols[2, at, :] = upright(meta[k, 0, t, 2:3, :])
            cols[3, at, :] = upright(meta[k, 1, t, 2:3, :])
            cols[4, at, :] = upright(share)

        with jax.named_scope("settle_wait"):
            swap(k, j).wait_recv()
        at = chunk(j)
        low = wide(quant[k, 0, at, :], cols[2, at, :])
        high = wide(quant[k, 1, at, :], cols[3, at, :])
        old = cents[at, :].astype(F32)
        fresh(k, j)[...] = ((low + high + old) * cols[4, at, :]).astype(BF16)
        down(k, j).start()
        spread(k, j)

    step = npoints // PIECES

    @jax.named_scope("near_start")
    def near_start(cents):
        cent = cents[...]
        csq[...] = jnp.sum(jnp.square(cent.astype(F32)), axis=1, keepdims=True)
        scaled[...] = (cent * (-2.0)).astype(BF16)
        squares[...] = jnp.zeros(squares.shape, F32)

    @jax.named_scope("near")
    def near_piece(k, data, i):
        at = span(i * step, step)
        rows_in = data[at, :]
        cross = lax.dot_general(scaled[...], rows_in, (((1,), (1,)), ((), ())),
                                preferred_element_type=F32)
        mins[k, :, at] = jnp.min(cross + csq[...], axis=0, keepdims=True)
        sq = jnp.square(rows_in.astype(F32))
        squares[...] += jnp.sum(sq.reshape(step // 8, 8, width), axis=0)

    tile = 128
    setups = 4

    @jax.named_scope("setup")
    def setup(i):
        for j in range(npoints // (tile * setups)):
            at = span(i * (npoints // setups) + j * tile, tile)
            column[at, :] = jnp.broadcast_to(code_one[:, at], (tile, tile)).T
        at = span(i * (npoints // setups), npoints // setups)
        residual[at, :] = points[at, :]

    halves = GROUP // SIZE
    looks = 2
    depth = GROUP * ncb
    look_step = 1024

    @jax.named_scope("look")
    def look(b, h):
        @pl.when(h == 0)
        def _():
            for jj in range(halves):
                for o in range(nx):
                    with jax.named_scope("d_wait"):
                        d_copy(o, b * halves + jj).wait_recv()

        labels = []
        for q in range(depth // tile):
            lane = q * tile + lax.broadcasted_iota(jnp.int32, (look_step, tile), 1)
            labels.append((lane // GROUP) * rows + lane % GROUP + b * GROUP)

        def one(s, carry):
            at = span(h * (npoints // looks) + s * look_step, look_step)
            held = column[at, :]
            hot = jnp.concatenate(
                [jnp.where(held == label, 1.0, 0.0).astype(BF16) for label in labels], axis=1
            )
            found = jnp.dot(hot, codebook[span(b * depth, depth), :], preferred_element_type=F32)
            residual[at, :] = (residual[at, :].astype(F32) - found).astype(BF16)
            return carry

        lax.fori_loop(0, npoints // (looks * look_step), one, 0)

    @jax.named_scope("totals")
    def totals():
        for d in range(1, ncb):
            min_copy(d).wait()
        best = mins[...]
        for d in range(1, ncb):
            best = jnp.minimum(best, mins_in[d])
        squares_two = jnp.sum(squares[...], keepdims=True)
        for k in range(2):
            sq = squares_two if k == 1 else tot[0, :, :1]
            tot[k] = jnp.broadcast_to(jnp.sum(best[k], keepdims=True) + sq, tot.shape[1:])
        for d in range(1, npts):
            tot_copy(d).start()

    def close_first(j):
        @pl.when(outer)
        def _():
            up(0, j).wait_send()

        @pl.when(inner)
        def _():
            swap(0, j).wait_send()
            down(0, j).wait_send()

        for o in range(nx):
            d_copy(o, j).wait_send()
            if o > 0:
                x_copy(o, j).wait_send()

    def close_meta(k):
        for t in range(rows // SPAN):
            @pl.when(outer)
            def _():
                meta_up(k, t).wait_send()

            @pl.when(inner)
            def _():
                meta_swap(k, t).wait_send()

    def exchange(k, data, cents):
        lag_join = LJ
        lag_settle = LS
        lag_down = LD
        lag_x = jnp.where(inner, LS, LD) + LX

        def run(i, carry):
            @pl.when(inner)
            def _():
                j = i - lag_settle

                @pl.when(jnp.logical_and(j >= 0, j < n))
                def _():
                    settle(k, j, cents)

                j = i - lag_join

                @pl.when(jnp.logical_and(j >= 0, j < n))
                def _():
                    join(k, j)

            @pl.when(outer)
            def _():
                j = i - lag_down

                @pl.when(jnp.logical_and(j >= 0, j < n))
                def _():
                    with jax.named_scope("down_wait"):
                        down(k, j).wait_recv()
                    spread(k, j)
                    if k == 1:
                        up(1, j).wait_send()

            @pl.when(i < PIECES)
            def _():
                near_piece(k, data, i)

            if k == 0:
                @pl.when(jnp.logical_and(i >= PIECES, i < PIECES + setups))
                def _():
                    setup(i - PIECES)

                j = i - lag_x

                @pl.when(jnp.logical_and(j >= 0, j < n))
                def _():
                    for o in range(1, nx):
                        with jax.named_scope("x_wait"):
                            x_copy(o, j).wait_recv()
                        d_copy(o, j).start()

                v = i - lag_x - LK

                every = halves // looks

                @pl.when(jnp.logical_and(v >= 0, jnp.logical_and(v < n, v % every == 0)))
                def _():
                    look(v // halves, (v % halves) // every)
            else:
                @pl.when(i < n)
                def _():
                    close_first(i)

                @pl.when(i == n)
                def _():
                    close_meta(0)

                @pl.when(i == PIECES)
                def _():
                    for d in range(1, ncb):
                        min_copy(d).start()

                @pl.when(i == PIECES + 6)
                def _():
                    totals()

            return carry

        steps = n + LD + LX + LK if k == 0 else n + LD
        lax.fori_loop(0, steps, run, 0)

    loads[0].wait()
    loads[1].wait()
    pieces_of_sums(0, points, code_one)
    loads[2].wait()
    loads[3].wait()
    loads[4].wait()
    near_start(cent_one)
    exchange(0, points, cent_one)
    tot[0] = jnp.broadcast_to(jnp.sum(squares[...], keepdims=True), tot.shape[1:])
    pieces_of_sums(1, residual, code_two)
    near_start(cent_two)
    for g in range(rows // GROUP):
        new_one[g * GROUP:(g + 1) * GROUP, :] = codebook[span(g * depth + c * GROUP, GROUP), :]
    exchange(1, residual, cent_two)

    @pl.when(inner)
    def _():
        def drain(j, carry):
            swap(1, j).wait_send()
            down(1, j).wait_send()
            return carry

        lax.fori_loop(0, n, drain, 0)

    close_meta(1)
    for d in range(1, npts):
        tot_copy(d).wait()
    tot_in[p] = tot[...]
    total = tot_in[0]
    for d in range(1, npts):
        total = total + tot_in[d]
    total_out[...] = total / F32(npoints * npts * width)


def finish_kernel(one_in, two_in, total_in, one_out, two_out, total_out, sem):
    first = pltpu.make_async_copy(one_in, one_out, sem.at[0])
    second = pltpu.make_async_copy(two_in, two_out, sem.at[1])
    first.start()
    second.start()
    for k in range(2):
        total_out[k] = jnp.sum(total_in[k, :, :1])
    first.wait()
    second.wait()


def finish(new_one, new_two, total):
    vmem = pl.BlockSpec(memory_space=pltpu.VMEM)
    anywhere = pl.BlockSpec(memory_space=pl.ANY)
    return pl.pallas_call(
        finish_kernel,
        out_shape=(
            jax.ShapeDtypeStruct(new_one.shape, BF16),
            jax.ShapeDtypeStruct(new_two.shape, BF16),
            jax.ShapeDtypeStruct((2,), F32),
        ),
        in_specs=[vmem] * 3,
        out_specs=(anywhere, anywhere, pl.BlockSpec(memory_space=pltpu.SMEM)),
        scratch_shapes=[pltpu.SemaphoreType.DMA((2,))],
        compiler_params=pltpu.CompilerParams(vmem_limit_bytes=8 * 1024 * 1024),
    )(new_one, new_two, total)


def fused(points, code_one, code_two, cent_one, cent_two):
    npts = lax.axis_size("pts")
    ncb = lax.axis_size("cb")
    npoints, width = points.shape
    rows = cent_one.shape[0]
    nx = ncb // CORES
    n = rows // SIZE
    spans = rows // SPAN
    vmem = pl.BlockSpec(memory_space=pltpu.VMEM)
    dma = pltpu.SemaphoreType.DMA
    new_one, new_two, total = pl.pallas_call(
        functools.partial(fused_kernel, npts, ncb),
        out_shape=(
            pltpu.VMEM(cent_one.shape, BF16),
            pltpu.VMEM(cent_two.shape, BF16),
            pltpu.VMEM((2, 1, 128), F32),
        ),
        in_specs=[pl.BlockSpec(memory_space=pl.ANY)] * 5,
        out_specs=(vmem,) * 3,
        scratch_shapes=[
            pltpu.VMEM(points.shape, BF16),
            pltpu.VMEM((1, npoints), jnp.int32),
            pltpu.VMEM((1, npoints), jnp.int32),
            pltpu.VMEM(cent_one.shape, BF16),
            pltpu.VMEM(cent_two.shape, BF16),
            dma((5,)),
            pltpu.VMEM(points.shape, BF16),
            pltpu.VMEM((rows * ncb, width), BF16),
            pltpu.VMEM((rows, width), F32),
            pltpu.VMEM((2, 2, rows, width), I16),
            pltpu.VMEM((2, rows, width), I16),
            pltpu.VMEM((2, 2, spans, 4, SPAN), F32),
            pltpu.VMEM((2, spans, 4, SPAN), F32),
            pltpu.VMEM((5, rows, 1), F32),
            pltpu.VMEM((2, spans, 1, SPAN), F32),
            pltpu.VMEM((npoints, 128), jnp.int32),
            pltpu.VMEM((2, 1, npoints), F32),
            pltpu.VMEM((ncb, 2, 1, npoints), F32),
            pltpu.VMEM((2, 1, 128), F32),
            pltpu.VMEM((npts, 2, 1, 128), F32),
            pltpu.VMEM((rows, width), BF16),
            pltpu.VMEM((rows, 1), F32),
            pltpu.VMEM((8, width), F32),
            dma((2, n)), dma((2, n)), dma((2, n)), dma((2, n)), dma((2, n)), dma((2, n)),
            dma((2, spans)), dma((2, spans)), dma((2, spans)), dma((2, spans)),
            dma((nx, n)), dma((nx, n)), dma((nx, n)), dma((nx, n)),
            dma((ncb,)), dma((ncb,)), dma((npts,)), dma((npts,)),
        ],
        compiler_params=pltpu.CompilerParams(
            collective_id=0, has_side_effects=True, vmem_limit_bytes=60 * 1024 * 1024
        ),
    )(points, code_one.reshape(1, npoints), code_two.reshape(1, npoints), cent_one, cent_two)
    return finish(new_one, new_two, total)


def nearest_local(data, cents):
    sq = jnp.sum(jnp.square(data.astype(jnp.float32)), axis=1)
    csq = jnp.sum(jnp.square(cents.astype(jnp.float32)), axis=1)
    cross = lax.dot_general(
        data, cents, (((1,), (1,)), ((), ())), preferred_element_type=jnp.float32
    )
    dist = sq[:, None] - 2.0 * cross + csq[None, :]
    local_min = jnp.min(dist, axis=1)
    best = lax.pmin(local_min, "cb")
    return jnp.sum(best)


def section_update(data, codes, cents):
    rows = cents.shape[0]
    first = lax.axis_index("cb") * rows
    labels = first + lax.broadcasted_iota(jnp.int32, (1, rows), 1)
    onehot = (codes[:, None] == labels).astype(jnp.bfloat16)
    sums = lax.dot_general(
        onehot, data, (((0,), (0,)), ((), ())), preferred_element_type=jnp.float32
    )
    counts = jnp.sum(onehot.astype(jnp.float32), axis=0)
    share_sums, share_counts = (
        lax.psum_scatter(sums, "pts", scatter_dimension=0, tiled=True),
        lax.psum_scatter(counts, "pts", scatter_dimension=0, tiled=True),
    )
    share_rows = share_sums.shape[0]
    old_rows = lax.dynamic_slice_in_dim(cents, lax.axis_index("pts") * share_rows, share_rows, 0)
    return ((share_sums + old_rows.astype(jnp.float32)) / (share_counts + 1.0)[:, None]).astype(
        jnp.bfloat16
    )


def section_total(value):
    return lax.psum(value, "pts")


def local(points, code_one, code_two, cent_one, cent_two):
    rows = cent_one.shape[0]
    width = points.shape[1]
    npts = lax.axis_size("pts")
    ncb = lax.axis_size("cb")
    first = lax.axis_index("cb") * rows
    first_local = nearest_local(points, cent_one)
    updated_one = section_update(points, code_one, cent_one)
    gathered = lax.all_gather(updated_one, ("pts", "cb"), axis=0, tiled=True)
    share_rows = updated_one.shape[0]
    codebook = jnp.swapaxes(gathered.reshape(npts, ncb, share_rows, width), 0, 1).reshape(
        rows * ncb, width
    )
    new_one = lax.dynamic_slice_in_dim(codebook, first, rows, 0)
    looked = jnp.take(codebook, code_one, axis=0)
    residual = (points.astype(jnp.float32) - looked.astype(jnp.float32)).astype(jnp.bfloat16)
    updated_two = section_update(residual, code_two, cent_two)
    new_two = lax.all_gather(updated_two, "pts", axis=0, tiled=True)
    second_local = nearest_local(residual, cent_two)
    first_sum = section_total(first_local)
    second_sum = section_total(second_local)
    scale = jnp.float32(points.shape[0] * npts * width)
    distortion = jnp.stack([first_sum, second_sum]) / scale
    return (new_one, new_two, distortion)


def choose(points, code_one, code_two, cent_one, cent_two):
    rows, npts, ncb = cent_one.shape[0], lax.axis_size("pts"), lax.axis_size("cb")
    fits = (
        npts == 4
        and ncb % CORES == 0
        and (ncb * GROUP) % 128 == 0
        and rows % SPAN == 0
        and points.shape[0] % 2048 == 0
    )
    form = fused if fits else local
    return form(points, code_one, code_two, cent_one, cent_two)


def solution(mesh):
    return jax.shard_map(
        choose,
        mesh=mesh,
        in_specs=(
            P(("groups", "pts"), None),
            P(("groups", "pts")),
            P(("groups", "pts")),
            P(("groups", "cb"), None),
            P(("groups", "cb"), None),
        ),
        out_specs=(P(("groups", "cb"), None), P(("groups", "cb"), None), P("groups")),
        check_vma=False,
    )
```
